32 devices in a mesh: ty: 4 (over x, core), tx: 8 (over z, y).
Axes of the slice: x: 2, y: 2, z: 4, core: 2. Of those that a mesh axis runs over, the one named last changes fastest.
Arguments:
- exposures: float32 [256, 128, 128], P(('ty', 'tx')), may hold values from -70 to 70
- point_spread: float32 [256, 31, 31], P(('ty', 'tx')), may hold values from 0.0001 to 1
- warp_steps: int32 [256, 2], P(('ty', 'tx')), may hold values from 0 to 3
- column: int32 [256, 1], P(('ty', 'tx')), may hold values from 0 to 7; in each aligned block of 8 rows (0 to 7, 8 to 15, ...) at most 2 rows name the same one
- block_cell: int32 [256], P(('ty', 'tx')), may hold values from 0 to 15
Outputs:
- solution: float32 [2048, 4096], P('ty', 'tx')
- residual: float32 [2048, 4096], P('ty', 'tx')
The draws below stay inside these ranges and needn't reach their ends.
Inputs may be any that keep to these rules, and one draw needn't show every extreme that they name: `column`: among the 8 frame blocks of one device (aligned blocks of 8 rows) no value occurs more than 2 times, and in some such block one value occurs exactly 2 times.
All inputs are finite; a program needn't handle non-finite values.
Results may differ from the reference program's by a relative error of at most 0.0042.
Values may be sent and summed in bfloat16 or wider, within the bound.
A program may use at most 192 MiB of HBM per device.

```python
import math
import jax
import jax.numpy as jnp
import numpy as np
from jax import lax

TILE = 512
FB_DEV = 8
BLOCK = 128
PSF = 31
SUB = 4
ITERS = 2
TAPS = 32
HALO = 16
WIN = 160
CELLS = 16
CAP = 2
FRAMES_ROW = 64
FRAMES = 256
NY = 2048
NX = 4096
N_TX = 8


def draw_exposures(key, part):
    position = jnp.arange(FRAMES, dtype=jnp.float32) / max(FRAMES - 1, 1)
    scales = 1.0 + 2.0 * position
    noise_field = jnp.clip(jax.random.normal(jax.random.fold_in(key, 17), (FRAMES, BLOCK, BLOCK), jnp.float32), -6.0, 6.0)
    return noise_field * scales[:, None, None]


def plant(values, own_key, smallest, high):
    spot = [jax.random.randint(jax.random.fold_in(own_key, axis), (), 0, length) for axis, length in enumerate(values.shape)]
    longest = values.shape.index(max(values.shape))
    next_to = spot[:longest] + [(spot[longest] + 1) % values.shape[longest]] + spot[longest + 1:]
    return values.at[tuple(spot)].set(smallest).at[tuple(next_to)].set(high)


def shard_levels(rng, shape, shards, least, top_value):
    level, own = 1.0, jax.random.fold_in(rng, 6)
    for dim, blocks in shards:
        steps = jnp.exp(jax.random.uniform(jax.random.fold_in(own, dim), (blocks,), jnp.float32, least / len(shards), top_value / len(shards)))
        level = level * jnp.repeat(steps, shape[dim] // blocks).reshape([-1 if axis == dim else 1 for axis in range(len(shape))])
    return level


def assign_block(key, own, number, rows, number_of, top, most, lean):
    order = jax.random.permutation(key, number_of)
    crowded, common = shares(number_of, rows * top, most, lean, True), shares(number_of, rows * top, most, lean, False)
    places = jnp.arange(number_of)

    def named(lengths, rotation):
        used = int((lengths > 0).sum())
        fixed = max(1, used // 4)
        moved = fixed + (places - fixed + rotation * (used - fixed)) % max(1, number_of - fixed)
        return jnp.zeros((number_of,), jnp.int32).at[order[jnp.where(places < fixed, places, moved)]].set(jnp.asarray(lengths, jnp.int32))

    lengths = jnp.where(number % 4 == 0, named(crowded, number // 4), named(common, number - number // 4 - 1))
    mixed = jax.random.permutation(jax.random.fold_in(own, 3), number_of)
    giver, receiver = mixed[0:number_of // 2 * 2:2], mixed[1:number_of // 2 * 2:2]
    slack = jnp.minimum(lengths[giver] - 1, most - lengths[receiver]) // 2
    slack = jnp.where((giver == order[0]) | (receiver == order[0]) | (lengths[receiver] == 0), 0, jnp.maximum(slack, 0))
    moved = jax.random.randint(jax.random.fold_in(own, 4), (number_of // 2,), 0, 1 << 20) % (slack + 1)
    lengths = lengths.at[giver].add(-moved).at[receiver].add(moved)
    members = jnp.searchsorted(jnp.cumsum(lengths), jnp.arange(rows * top), side="right").astype(jnp.int32)
    table = members.reshape(top, rows).T
    table = table[jax.random.permutation(jax.random.fold_in(own, 1), rows)]
    rotation = jax.random.randint(jax.random.fold_in(own, 2), (rows, 1), 0, top)
    return jnp.take_along_axis(table, (jnp.arange(top)[None, :] + rotation) % top, axis=1)


def shares(number_of, total, bound, skew, full):
    weights = [(1 << 20) // math.isqrt(rank ** skew) + 1 for rank in range(1, number_of + 1)]
    largest = bound if full else min(bound, max(-(-total // number_of), total * weights[0] // sum(weights)))
    least = 1 if total - largest >= number_of - 1 else 0
    counts, spare = [largest] + [least] * (number_of - 1), total - largest - least * (number_of - 1)
    while spare > 0:
        candidates = [i for i in range(1, number_of) if counts[i] < largest] or [i for i in range(1, number_of) if counts[i] < bound]
        mass, left = sum([weights[i] for i in candidates]), spare
        for i in candidates:
            extra = min(bound - counts[i], max(1, left * weights[i] // mass), spare)
            counts[i] = counts[i] + extra
            spare = spare - extra
    return np.array(counts)


def setup_inputs(seed: int = 0) -> dict:
    arg_keys = jax.random.split(jax.random.key(seed), 6)
    exposures = draw_exposures(jax.random.fold_in(arg_keys[5], 71), 0)
    point_spread = jnp.clip(jnp.exp(math.log(1.0) - 9.2103404 * jax.random.uniform(arg_keys[1], (FRAMES, PSF, PSF), jnp.float32) ** shard_levels(arg_keys[1], (FRAMES, PSF, PSF), ((0, 32),), -0.2, 0.2)), 0.0001, 1.0)
    warp_steps = plant(jax.random.randint(arg_keys[2], (FRAMES, 2), 0, SUB), jax.random.fold_in(arg_keys[2], 1), 0, SUB - 1).astype(jnp.int32)
    column_keys = jax.random.split(jax.random.fold_in(arg_keys[3], 1), FRAMES // FB_DEV)
    column_turns = jax.random.permutation(jax.random.fold_in(arg_keys[3], 3), FRAMES // FB_DEV)
    column = jax.vmap(lambda own, number: assign_block(jax.random.fold_in(arg_keys[3], 2), own, number, FB_DEV, N_TX, 1, CAP, 2))(column_keys, column_turns).reshape((FRAMES, 1))
    block_cell = plant(jax.random.randint(arg_keys[4], (FRAMES,), 0, CELLS), jax.random.fold_in(arg_keys[4], 1), 0, CELLS - 1).astype(jnp.int32)
    return dict(exposures=exposures, point_spread=point_spread, warp_steps=warp_steps, column=column, block_cell=block_cell)


damping = 0.05


def make_kernels(point_spread, warp_steps):
    tap_count = point_spread.shape[-1] + 1
    totals = jnp.sum(point_spread, axis=(1, 2), keepdims=True)
    padded = jnp.pad(point_spread / totals, ((0, 0), (0, 1), (0, 1)))
    row_frac = (warp_steps[:, 0].astype(jnp.float32) / SUB)[:, None, None]
    col_frac = (warp_steps[:, 1].astype(jnp.float32) / SUB)[:, None, None]
    shifted = jnp.pad(padded, ((0, 0), (0, 0), (1, 0)))[:, :, :tap_count]
    blended = (1.0 - col_frac) * padded + col_frac * shifted
    lowered = jnp.pad(blended, ((0, 0), (1, 0), (0, 0)))[:, :tap_count, :]
    kernel = (1.0 - row_frac) * blended + row_frac * lowered
    return lax.optimization_barrier(kernel.astype(jnp.bfloat16)).astype(jnp.float32)


def rounded(values):
    return lax.optimization_barrier(values.astype(jnp.bfloat16)).astype(jnp.float32)


def window_anchors(column, block_cell):
    frame_index = jnp.arange(FRAMES, dtype=jnp.int32)
    per_row = TILE // BLOCK
    top_rows = (frame_index // FRAMES_ROW) * TILE + (block_cell.astype(jnp.int32) // per_row) * BLOCK
    left_cols = column[:, 0].astype(jnp.int32) * TILE + (block_cell.astype(jnp.int32) % per_row) * BLOCK
    return top_rows.astype(jnp.int32), left_cols.astype(jnp.int32)


def tap_table():
    taps_index = jnp.arange(TAPS)[:, None, None]
    positions = jnp.arange(WIN)[:, None]
    columns = jnp.arange(BLOCK)[None, :]
    table = jnp.where(positions - columns == taps_index, 1.0, 0.0).astype(jnp.float32)
    return table.reshape(TAPS, WIN * BLOCK)


def frame_bands(kernel_one, table):
    return jnp.dot(kernel_one, table, precision=lax.Precision.HIGHEST).reshape(TAPS, WIN, BLOCK)


def grouped(arrays):
    return tuple(member.reshape((FRAMES // FB_DEV, FB_DEV) + member.shape[1:]) for member in arrays)


def forward_all(field, kernels, top_rows, left_cols, table):
    padded = jnp.pad(field, HALO)

    def one_frame(kernel_one, top_row, left_col):
        framed = lax.dynamic_slice(padded, (top_row, left_col), (WIN, WIN))
        bands = frame_bands(kernel_one, table)
        stacked = jnp.stack([framed[offset:offset + BLOCK] for offset in range(TAPS)])
        return jnp.einsum('ayp,apx->yx', stacked, bands, precision=lax.Precision.HIGHEST)

    def one_group(operands):
        return jax.vmap(one_frame)(operands[0], operands[1], operands[2])

    result = lax.map(one_group, grouped((kernels, top_rows, left_cols)))
    return result.reshape(FRAMES, BLOCK, BLOCK)


def adjoint_all(images, kernels, top_rows, left_cols, table):
    def one_frame(frame_image, kernel_one):
        bands = frame_bands(kernel_one, table)
        spread = jnp.einsum('yx,apx->ayp', frame_image, bands, precision=lax.Precision.HIGHEST)
        summed = jnp.zeros((WIN, WIN), spread.dtype)
        for offset in range(TAPS):
            summed = summed + jnp.pad(spread[offset], ((offset, WIN - BLOCK - offset), (0, 0)))
        return summed

    def one_group(operands):
        return jax.vmap(one_frame)(operands[0], operands[1])

    patches = lax.map(one_group, grouped((images, kernels))).reshape(FRAMES, WIN, WIN)
    initial = jnp.zeros((NY + 2 * HALO, NX + 2 * HALO), patches.dtype)

    def place(slot_number, accumulated):
        current = lax.dynamic_slice(accumulated, (top_rows[slot_number], left_cols[slot_number]), (WIN, WIN))
        return lax.dynamic_update_slice(accumulated, current + patches[slot_number], (top_rows[slot_number], left_cols[slot_number]))

    accumulated = lax.fori_loop(0, FRAMES, place, initial)
    return accumulated[HALO:HALO + NY, HALO:HALO + NX]


def reference(exposures, point_spread, warp_steps, column, block_cell):
    kernels = make_kernels(point_spread, warp_steps)
    table = tap_table()
    top_rows, left_cols = window_anchors(column, block_cell)
    right_side = adjoint_all(rounded(exposures), kernels, top_rows, left_cols, table)
    solution = jnp.zeros_like(right_side)
    residual = right_side
    direction = right_side
    norm_now = jnp.sum(residual * residual)
    for iteration in range(ITERS):
        modelled = forward_all(rounded(direction), kernels, top_rows, left_cols, table)
        applied = adjoint_all(rounded(modelled), kernels, top_rows, left_cols, table) + damping * direction
        step_size = norm_now / jnp.sum(direction * applied)
        solution = solution + step_size * direction
        residual = residual - step_size * applied
        if iteration + 1 < ITERS:
            norm_next = jnp.sum(residual * residual)
            direction = residual + (norm_next / norm_now) * direction
            norm_now = norm_next
    return solution, residual
```

```python
import functools

import jax
import jax.numpy as jnp
from jax import lax
from jax.experimental import pallas as pl
from jax.experimental.pallas import tpu as pltpu
from jax.sharding import PartitionSpec as P

TILE = 512
SUB = 4
LANES = 128
GROUP = 32
MARGIN = 16
CAP = 2
EDGE = 2 * MARGIN
EXTENT = TILE + EDGE
PATCH = LANES + EDGE
ROWS = 144
PAD = 16
WIRE = jnp.bfloat16
SIDES = ((-1, 0), (1, 0), (0, -1), (0, 1), (-1, -1), (-1, 1), (1, -1), (1, 1))

damping = 0.05


def turn(value, shift):
    return pltpu.roll(value, shift % LANES, 1) if shift % LANES else value


def lanes_of(shape):
    return lax.broadcasted_iota(jnp.int32, shape, len(shape) - 1)


def pick_groups(parts):
    groups = lanes_of(parts[0].shape) >> 5
    value = parts[-1]
    for number in range(len(parts) - 2, -1, -1):
        value = jnp.where(groups == number, parts[number], value)
    return value


def make_taps(spread_ref, warp_ref, pad_ref, taps_ref, frame):
    pad_ref[frame] = jnp.zeros(pad_ref.shape[1:], jnp.float32)
    side = spread_ref.shape[1]
    pad_ref[frame, 8 : 8 + side, 0:side] = spread_ref[frame]
    shape = (GROUP, LANES)
    row_frac = jnp.full(shape, warp_ref[frame, 0], jnp.int32).astype(jnp.float32) / SUB
    col_frac = jnp.full(shape, warp_ref[frame, 1], jnp.int32).astype(jnp.float32) / SUB
    here = pad_ref[frame, 8 : 8 + GROUP]
    total = jnp.sum(jnp.sum(here, axis=0, keepdims=True), axis=1, keepdims=True)
    here = here / total
    above = pad_ref[frame, 7 : 7 + GROUP] / total
    here = (1.0 - col_frac) * here + col_frac * turn(here, 1)
    above = (1.0 - col_frac) * above + col_frac * turn(above, 1)
    pad_ref[frame, 8 : 8 + GROUP] = (1.0 - row_frac) * here + row_frac * above
    parts = []
    for part in range(4):
        near = pad_ref[frame, 8 + 8 * part : 12 + 8 * part]
        far = pad_ref[frame, 12 + 8 * part : 16 + 8 * part]
        parts.append(near + turn(far, 64))
    for part in range(4):
        pad_ref[frame, 8 + 4 * part : 12 + 4 * part] = parts[part]
    taps_ref[frame] = pad_ref[frame, 8:24].astype(jnp.bfloat16)


def toeplitz(rows):
    tiles = []
    for j in range(8):
        halves = []
        for half in range(2):
            row = rows[8 * half + j : 8 * half + j + 1]
            spread = jnp.broadcast_to(row, (GROUP, LANES))
            halves.append(pltpu.roll(spread, 0, 1, stride=1, stride_axis=0))
        tiles.append(jnp.concatenate(halves, axis=1))
    return jnp.concatenate(tiles, axis=0).astype(jnp.bfloat16)


def blur(shifted_ref, first, matrix, joined_ref):
    for g in range(4):
        near = shifted_ref[first + g, :ROWS]
        far = shifted_ref[first + g, PATCH - ROWS :]
        product = lax.dot_general(
            jnp.concatenate([near, far], axis=1),
            matrix,
            (((1,), (1,)), ((), ())),
            preferred_element_type=jnp.float32,
        )
        joined_ref[g] = product[: ROWS - 8, :LANES] + product[8:, LANES:]
    total = None
    for step in range(4):
        chosen = pick_groups([joined_ref[(j + step) % 4, j : j + LANES] for j in range(4)])
        chosen = turn(chosen, 32 * step)
        total = chosen if total is None else total + chosen
    return total


def hold_turns(image, turned_ref):
    for step in range(4):
        turned_ref[step, PAD : PAD + LANES] = turn(image, 32 * step)


def blur_back(turned_ref, matrix, behind_ref):
    low = lanes_of((PATCH, LANES)) < 64
    folded = []
    for h in range(4):
        rows = pick_groups(
            [turned_ref[(j - h) % 4, PAD - 8 - j : PAD - 8 - j + ROWS + 8] for j in range(4)]
        )
        stacked = jnp.concatenate(
            [rows[8:].astype(jnp.bfloat16), rows[:ROWS].astype(jnp.bfloat16)], axis=1
        )
        product = jnp.dot(stacked, matrix, preferred_element_type=jnp.float32)
        near, far = product[:, :LANES], product[:, LANES:]
        folded.append(jnp.concatenate([near[:16], near[16:] + far[: ROWS - 16], far[ROWS - 16 :]], axis=0))
    sums = []
    for number in range(2):
        one, two = folded[number], folded[number + 2]
        behind_ref[number, 8 : 8 + PATCH] = jnp.where(low, turn(one, 64), two)
        ahead = jnp.where(low, one, turn(two, 64))
        sums.append(ahead + behind_ref[number, 4 : 4 + PATCH])
    moved = turn(sums[1], 32)
    wrapped = lanes_of(moved.shape) < GROUP
    return sums[0] + jnp.where(wrapped, 0.0, moved), jnp.where(wrapped, moved, 0.0)


def assemble(running_ref, index_ref, per_row, field_ref):
    block = LANES

    def part(row, col, side, first, count):
        if 0 <= row < per_row and 0 <= col < per_row:
            return [running_ref[index_ref[row * per_row + col], side, first : first + count]]
        return []

    for row in range(per_row + 1):
        for col in range(per_row + 1):
            both = part(row - 1, col, 0, block, EDGE) + part(row - 1, col - 1, 1, block, EDGE)
            rest = part(row, col, 0, 0, EDGE) + part(row, col - 1, 1, 0, EDGE)
            field_ref[col, row * block : row * block + EDGE] = sum((both + rest)[1:], (both + rest)[0])
            if row < per_row:
                count = block - EDGE
                body = part(row, col, 0, EDGE, count) + part(row, col - 1, 1, EDGE, count)
                field_ref[col, row * block + EDGE : (row + 1) * block] = sum(body[1:], body[0])


def flat_strip(strip_ref, tile):
    height = EXTENT // 4
    parts = [turn(strip_ref[tile, k * height : (k + 1) * height], 32 * k) for k in range(4)]
    return pick_groups(parts).astype(WIRE)


def add_flat(field_ref, tile, flat):
    height = EXTENT // 4
    wrapped = lanes_of((height, LANES)) < GROUP
    flat = flat.astype(jnp.float32)
    for k in range(4):
        rows = slice(k * height, (k + 1) * height)
        field_ref[tile, rows] += jnp.where(wrapped, turn(flat, -32 * k), 0.0)


def shift_field(field_ref, shifted_ref, per_row, sums_ref, row):
    chunk = 16

    tall = PATCH // chunk

    @pl.loop(0, per_row * tall)
    def _(step):
        number = step // tall * (LANES // chunk) + lax.rem(step, tall)
        start = pl.multiple_of(number * chunk, chunk)
        local = pl.multiple_of(lax.rem(step, tall) * chunk, chunk)
        cell = step // tall * per_row
        lanes = lanes_of((chunk, LANES))
        low, middle = lanes < 64, (lanes >= 32) & (lanes < 96)
        now = [field_ref[col, pl.ds(start, chunk)] for col in range(per_row + 1)]
        later = [field_ref[col, pl.ds(start + 4, chunk)] for col in range(per_row + 1)]
        by96 = [turn(jnp.where(middle, a, b), 96) for a, b in zip(now, later)]
        by32 = [turn(jnp.where(middle, b, a), 32) for a, b in zip(now, later)]
        for col in range(per_row):
            a, b = now[col], later[col]
            by64 = turn(jnp.where(low, b, a), 64)
            parts = [
                jnp.where(low, a, by64),
                jnp.where(low, by96[col], by32[col]),
                jnp.where(low, by64, b),
                pick_groups([by32[col], by32[col + 1], by96[col], by96[col + 1]]),
            ]
            for g in range(4):
                shifted_ref[4 * (cell + col) + g, pl.ds(local, chunk)] = parts[g].astype(jnp.bfloat16)
        squares = None
        for col in range(per_row + 1):
            value = now[col]
            if col == 0:
                value = jnp.where(lanes < MARGIN, 0.0, value)
            if col == per_row:
                value = jnp.where(lanes < MARGIN, value, 0.0)
            squares = value * value if squares is None else squares + value * value
        once = (lax.rem(step, tall) < LANES // chunk) | (cell == per_row * (per_row - 1))
        inside = once & (number >= MARGIN // chunk) & (number < EXTENT // chunk - MARGIN // chunk)
        sums_ref[row] += jnp.where(inside, squares[:8] + squares[8:], 0.0)


def whole_kernel(
    sizes,
    exposures_ref,
    spread_ref,
    warp_ref,
    column_ref,
    cell_ref,
    solution_ref,
    residual_ref,
    pad_ref,
    taps_ref,
    send_ref,
    frames_ref,
    tag_send_ref,
    tags_ref,
    tag_smem,
    key_smem,
    order_smem,
    index_smem,
    matrix_ref,
    patch_ref,
    running_ref,
    turned_ref,
    behind_ref,
    joined_ref,
    shifted_ref,
    field_ref,
    row_send_ref,
    col_send_ref,
    row_land_ref,
    col_land_ref,
    corner_land_ref,
    sums_ref,
    total_ref,
    ty_land_ref,
    tx_land_ref,
    tag_sems,
    frame_sems,
    local_sem,
    halo_sems,
    ty_sems,
    tx_sems,
):
    ty_size, tx_size = sizes
    frame_count, block = exposures_ref.shape[:2]
    per_row = TILE // block
    cells = per_row * per_row
    slots = CAP * tx_size
    ty, tx = lax.axis_index("ty"), lax.axis_index("tx")

    def has(side):
        row, col = side
        ok = None
        for step, place, size in ((row, ty, ty_size), (col, tx, tx_size)):
            test = (place > 0) if step < 0 else (place < size - 1) if step > 0 else None
            if test is not None:
                ok = test if ok is None else ok & test
        return ok

    def at(side):
        return {"ty": ty + side[0], "tx": tx + side[1]}

    barrier = pltpu.get_barrier_semaphore()

    def greet(device):
        pl.semaphore_signal(barrier, inc=1, device_id=device, device_id_type=pl.DeviceIdType.MESH)

    for step in range(1, tx_size):
        greet({"tx": lax.rem(tx + step, tx_size)})
    for step in range(1, ty_size):
        greet({"ty": lax.rem(ty + step, ty_size)})
    for side in SIDES[4:]:
        pl.when(has(side))(functools.partial(greet, at(side)))

    for frame in range(frame_count):
        make_taps(spread_ref, warp_ref, pad_ref, taps_ref, frame)

    running_ref[0] = jnp.zeros(running_ref.shape[1:], jnp.float32)
    turned_ref[...] = jnp.zeros_like(turned_ref)
    behind_ref[...] = jnp.zeros_like(behind_ref)
    sums_ref[...] = jnp.zeros_like(sums_ref)
    for number in range(3):
        field_ref[number, :, EXTENT:] = jnp.zeros((per_row + 1, 8, LANES), jnp.float32)

    peers = tx_size - 1 + ty_size - 1
    for side in SIDES[4:]:
        peers = peers + jnp.where(has(side), 1, 0)
    pl.semaphore_wait(barrier, peers)

    def sources(target):
        first, second, count = jnp.int32(0), jnp.int32(0), jnp.int32(0)
        for frame in range(frame_count):
            match = column_ref[frame_count - 1 - frame] == target
            first = jnp.where(match, frame_count - 1 - frame, first)
            second = jnp.where(column_ref[frame] == target, frame, second)
            count = count + jnp.where(match, 1, 0)
        return first, second, count

    def tag_copy(step):
        return pltpu.make_async_remote_copy(
            src_ref=tag_send_ref.at[step],
            dst_ref=tags_ref.at[step],
            send_sem=tag_sems.at[0, step],
            recv_sem=tag_sems.at[1, step],
            device_id={"tx": lax.rem(tx + step, tx_size)},
            device_id_type=pl.DeviceIdType.MESH,
        )

    def frame_copy(step):
        return pltpu.make_async_remote_copy(
            src_ref=send_ref.at[step],
            dst_ref=frames_ref.at[step],
            send_sem=frame_sems.at[0, step],
            recv_sem=frame_sems.at[1, step],
            device_id={"tx": lax.rem(tx + step, tx_size)},
            device_id_type=pl.DeviceIdType.MESH,
        )

    def tags_for(step):
        first, second, count = sources(lax.rem(tx + step, tx_size))
        one = jnp.where(count >= 1, cell_ref[first], -1)
        two = jnp.where(count >= 2, cell_ref[second], -1)
        shape = tags_ref.shape[1:]
        rows = lax.broadcasted_iota(jnp.int32, shape, 0)
        return jnp.where(rows == 0, jnp.full(shape, one, jnp.int32), jnp.full(shape, two, jnp.int32))

    def fill(ref, step):
        first, second, _ = sources(lax.rem(tx + step, tx_size))
        for number, origin in enumerate((first, second)):
            ref[step, number, :block] = exposures_ref[origin].astype(jnp.bfloat16)
            ref[step, number, block:] = taps_ref[origin]

    tags_ref[0] = tags_for(0)

    @pl.loop(1, tx_size)
    def _(step):
        tag_send_ref[step] = tags_for(step)
        tag_copy(step).start()

    @pl.loop(1, tx_size)
    def _(step):
        fill(send_ref, step)
        frame_copy(step).start()

    fill(frames_ref, 0)

    def first_pass(step):
        for number in range(CAP):
            slot = CAP * step + number
            matrix = toeplitz(frames_ref[step, number, block:].astype(jnp.float32))
            matrix_ref[slot] = matrix
            hold_turns(frames_ref[step, number, :block].astype(jnp.float32), turned_ref)
            left, right = blur_back(turned_ref, matrix, behind_ref)
            patch_ref[slot, 0] = left
            patch_ref[slot, 1] = right

    first_pass(0)

    @pl.loop(1, tx_size)
    def _(step):
        tag_copy(step).wait()

    local = pltpu.make_async_copy(tags_ref, tag_smem, local_sem)
    local.start()
    local.wait()

    @pl.loop(0, slots)
    def _(slot):
        key_smem[slot] = tag_smem[slot // CAP, lax.rem(slot, CAP), 0] * slots + slot

    @pl.loop(0, slots)
    def _(slot):
        key = key_smem[slot]
        rank = jnp.int32(0)
        for other in range(slots):
            rank = rank + jnp.where(key_smem[other] < key, 1, 0)
        order_smem[0, slot] = rank

    @pl.loop(0, slots)
    def _(place):
        slot = jnp.int32(0)
        for other in range(slots):
            slot = jnp.where(order_smem[0, other] == place, other, slot)
        order_smem[1, place] = slot
        cell = tag_smem[slot // CAP, lax.rem(slot, CAP), 0]
        order_smem[2, place] = cell

    @pl.loop(0, cells)
    def _(cell):
        upto, equal = jnp.int32(0), jnp.int32(0)
        for place in range(slots):
            value = order_smem[2, place]
            upto = upto + jnp.where(value <= cell, 1, 0)
            equal = equal + jnp.where(value == cell, 1, 0)
        index_smem[cell] = jnp.where(equal > 0, upto, 0)

    @pl.loop(1, tx_size)
    def _(step):
        frame_copy(step).wait()
        first_pass(step)

    def same(place):
        before = order_smem[2, jnp.maximum(place - 1, 0)]
        return (place > 0) & (before == order_smem[2, place])

    @pl.loop(0, slots)
    def _(place):
        kept = same(place)
        slot = order_smem[1, place]
        for side in range(2):
            running_ref[place + 1, side] = patch_ref[slot, side] + jnp.where(
                kept, running_ref[place, side], 0.0
            )

    def halo_copy(turn_number, which):
        row, col = SIDES[which]
        if col == 0:
            source = row_send_ref.at[turn_number, (row + 1) // 2]
            target = row_land_ref.at[turn_number, (1 - row) // 2]
        elif row == 0:
            source = col_send_ref.at[turn_number, (col + 1) // 2]
            target = col_land_ref.at[turn_number, (1 - col) // 2]
        else:
            source = row_send_ref.at[turn_number, (row + 1) // 2, per_row * ((col + 1) // 2)]
            target = corner_land_ref.at[turn_number, (1 - row) // 2, (1 - col) // 2]
        return pltpu.make_async_remote_copy(
            src_ref=source,
            dst_ref=target,
            send_sem=halo_sems.at[0, turn_number, which],
            recv_sem=halo_sems.at[1, turn_number, SIDES.index((-row, -col))],
            device_id=at(SIDES[which]),
            device_id_type=pl.DeviceIdType.MESH,
        )

    def share_edges(number):
        own = field_ref.at[number]
        for end in range(2):
            col_send_ref[number, end] = flat_strip(own, per_row * end)
        for which in (2, 3):
            pl.when(has(SIDES[which]))(lambda which=which: halo_copy(number, which).start())
        for end in range(2):
            for col in range(per_row + 1):
                row_send_ref[number, end, col] = own[col, TILE * end : TILE * end + EDGE].astype(WIRE)
        for which in (4, 5, 6, 7, 0, 1):
            pl.when(has(SIDES[which]))(lambda which=which: halo_copy(number, which).start())

    def take_edges(number):
        own = field_ref.at[number]

        def land(which):
            row, col = SIDES[which]
            halo_copy(number, which).wait_send()
            back = SIDES.index((row, col))
            pltpu.make_async_remote_copy(
                src_ref=halo_source(which),
                dst_ref=halo_target(which),
                send_sem=halo_sems.at[0, number, which],
                recv_sem=halo_sems.at[1, number, back],
                device_id=at(SIDES[which]),
                device_id_type=pl.DeviceIdType.MESH,
            ).wait_recv()
            if col == 0:
                end = (row + 1) // 2
                for tile in range(per_row + 1):
                    own[tile, TILE * end : TILE * end + EDGE] += row_land_ref[number, end, tile].astype(
                        jnp.float32
                    )
            elif row == 0:
                end = (col + 1) // 2
                add_flat(own, per_row * end, col_land_ref[number, end])
            else:
                end, tile = (row + 1) // 2, per_row * ((col + 1) // 2)
                value = corner_land_ref[number, end, (col + 1) // 2].astype(jnp.float32)
                inside = lanes_of(value.shape) < EDGE
                own[tile, TILE * end : TILE * end + EDGE] += jnp.where(inside, value, 0.0)

        def halo_source(which):
            row, col = SIDES[which]
            if col == 0:
                return row_send_ref.at[number, (row + 1) // 2]
            if row == 0:
                return col_send_ref.at[number, (col + 1) // 2]
            return row_send_ref.at[number, (row + 1) // 2, per_row * ((col + 1) // 2)]

        def halo_target(which):
            row, col = SIDES[which]
            if col == 0:
                return row_land_ref.at[number, (row + 1) // 2]
            if row == 0:
                return col_land_ref.at[number, (col + 1) // 2]
            return corner_land_ref.at[number, (row + 1) // 2, (col + 1) // 2]

        for which in range(len(SIDES)):
            pl.when(has(SIDES[which]))(functools.partial(land, which))

    def clear_outside(number):
        own = field_ref.at[number]

        @pl.when(ty == 0)
        def _():
            for tile in range(per_row + 1):
                own[tile, :MARGIN] = jnp.zeros((MARGIN, LANES), jnp.float32)

        @pl.when(ty == ty_size - 1)
        def _():
            for tile in range(per_row + 1):
                own[tile, TILE + MARGIN : EXTENT] = jnp.zeros((MARGIN, LANES), jnp.float32)

        @pl.when(tx == 0)
        def _():
            value = own[0, :EXTENT]
            own[0, :EXTENT] = jnp.where(lanes_of(value.shape) < MARGIN, 0.0, value)

        @pl.when(tx == tx_size - 1)
        def _():
            value = own[per_row, :EXTENT]
            own[per_row, :EXTENT] = jnp.where(lanes_of(value.shape) < MARGIN, value, 0.0)

    def gather_field(number):
        assemble(running_ref, index_smem, per_row, field_ref.at[number])
        share_edges(number)

    def damp(number):
        for tile in range(per_row + 1):
            field_ref[number, tile, :EXTENT] += damping * field_ref[number - 1, tile, :EXTENT]

    def normal_pass(row):
        @pl.loop(0, slots)
        def _(place):
            slot = order_smem[1, place]
            cell = order_smem[2, place]
            valid = cell >= 0
            cell = jnp.maximum(cell, 0)
            kept = same(place)
            matrix = matrix_ref[slot]
            modelled = blur(shifted_ref, cell * 4, matrix, joined_ref)
            squares = modelled * modelled
            squares = squares.reshape(block // 8, 8, LANES).sum(axis=0)
            sums_ref[row] += jnp.where(valid, squares, 0.0)
            hold_turns(modelled.astype(jnp.bfloat16).astype(jnp.float32), turned_ref)
            left, right = blur_back(turned_ref, matrix, behind_ref)
            running_ref[place + 1, 0] = left + jnp.where(kept, running_ref[place, 0], 0.0)
            running_ref[place + 1, 1] = right + jnp.where(kept, running_ref[place, 1], 0.0)

    gather_field(0)
    take_edges(0)
    clear_outside(0)
    shift_field(field_ref.at[0], shifted_ref, per_row, sums_ref, 0)
    normal_pass(1)
    gather_field(1)
    take_edges(1)
    clear_outside(1)
    damp(1)
    shift_field(field_ref.at[1], shifted_ref, per_row, sums_ref, 2)
    normal_pass(3)

    def sum_copies(axis, place, size, source, landed, sems):
        return [
            pltpu.make_async_remote_copy(
                src_ref=source,
                dst_ref=landed.at[step - 1],
                send_sem=sems.at[0, step - 1],
                recv_sem=sems.at[1, step - 1],
                device_id={axis: lax.rem(place + step, size)},
                device_id_type=pl.DeviceIdType.MESH,
            )
            for step in range(1, size)
        ]

    rows = lax.broadcasted_iota(jnp.int32, (8, LANES), 0)
    packed = jnp.zeros((8, LANES), jnp.float32)
    for number in range(4):
        packed = jnp.where(rows == number, jnp.sum(sums_ref[number], axis=0, keepdims=True), packed)
    total_ref[0] = packed
    ty_copies = sum_copies("ty", ty, ty_size, total_ref.at[0], ty_land_ref, ty_sems)
    for copy in ty_copies:
        copy.start()
    assemble(running_ref, index_smem, per_row, field_ref.at[2])
    share_edges(2)
    for copy in ty_copies:
        copy.wait()
    partial = total_ref[0]
    for step in range(ty_size - 1):
        partial = partial + ty_land_ref[step]
    total_ref[1] = partial
    tx_copies = sum_copies("tx", tx, tx_size, total_ref.at[1], tx_land_ref, tx_sems)
    for copy in tx_copies:
        copy.start()
    take_edges(2)
    damp(2)
    for copy in tx_copies:
        copy.wait()
    partial = total_ref[1]
    for step in range(tx_size - 1):
        partial = partial + tx_land_ref[step]
    sums = jnp.broadcast_to(jnp.sum(partial, axis=1, keepdims=True), (8, LANES))
    r00 = sums[0:1]
    r01 = sums[1:2] + damping * r00
    r11 = sums[2:3]
    r12 = sums[3:4] + damping * r11
    step0 = r00 / r01
    norm_next = r00 - 2.0 * step0 * r01 + step0 * step0 * r11
    grown = 1.0 + norm_next / r00
    curvature = grown * grown * r01 - 2.0 * grown * step0 * r11 + step0 * step0 * r12
    step1 = norm_next / curvature
    x0 = step0 + step1 * grown
    x1 = -step1 * step0
    y1 = -step0 - step1 * grown
    y2 = step1 * step0

    chunk = 32

    @pl.loop(0, TILE // chunk)
    def _(number):
        start = pl.multiple_of(number * chunk, chunk)
        source = pl.ds(pl.multiple_of(start + MARGIN, 8), chunk)
        inside = lanes_of((chunk, LANES)) < LANES - MARGIN
        solved, left = [], []
        for tile in range(per_row + 1):
            q0, q1, q2 = (field_ref[k, tile, source] for k in range(3))
            solved.append(turn(x0 * q0 + x1 * q1, -MARGIN))
            left.append(turn(q0 + y1 * q1 + y2 * q2, -MARGIN))
        for tile in range(per_row):
            lanes = slice(tile * LANES, (tile + 1) * LANES)
            solution_ref[pl.ds(start, chunk), lanes] = jnp.where(inside, solved[tile], solved[tile + 1])
            residual_ref[pl.ds(start, chunk), lanes] = jnp.where(inside, left[tile], left[tile + 1])


def body(exposures, point_spread, warp_steps, column, block_cell):
    ty_size, tx_size = lax.axis_size("ty"), lax.axis_size("tx")
    frame_count, block = exposures.shape[:2]
    per_row = TILE // block
    slots = CAP * tx_size
    tall = EXTENT + 8
    f32, bf16 = jnp.float32, jnp.bfloat16
    vmem = pl.BlockSpec(memory_space=pltpu.VMEM)
    smem = pl.BlockSpec(memory_space=pltpu.SMEM)
    dma = pltpu.SemaphoreType.DMA
    scratch = [
        pltpu.VMEM((frame_count, 48, LANES), f32),
        pltpu.VMEM((frame_count, 16, LANES), bf16),
        pltpu.VMEM((tx_size, CAP, ROWS, LANES), bf16),
        pltpu.VMEM((tx_size, CAP, ROWS, LANES), bf16),
        pltpu.VMEM((tx_size, 8, LANES), jnp.int32),
        pltpu.VMEM((tx_size, 8, LANES), jnp.int32),
        pltpu.SMEM((tx_size, 8, LANES), jnp.int32),
        pltpu.SMEM((slots,), jnp.int32),
        pltpu.SMEM((3, slots), jnp.int32),
        pltpu.SMEM((per_row * per_row,), jnp.int32),
        pltpu.VMEM((slots, 256, 256), bf16),
        pltpu.VMEM((slots, 2, PATCH, LANES), f32),
        pltpu.VMEM((slots + 1, 2, PATCH, LANES), f32),
        pltpu.VMEM((4, PAD + ROWS, LANES), f32),
        pltpu.VMEM((2, 8 + PATCH, LANES), f32),
        pltpu.VMEM((4, ROWS - 8, LANES), f32),
        pltpu.VMEM((4 * per_row * per_row, PATCH, LANES), bf16),
        pltpu.VMEM((3, per_row + 1, tall, LANES), f32),
        pltpu.VMEM((3, 2, per_row + 1, EDGE, LANES), WIRE),
        pltpu.VMEM((3, 2, EXTENT // 4, LANES), WIRE),
        pltpu.VMEM((3, 2, per_row + 1, EDGE, LANES), WIRE),
        pltpu.VMEM((3, 2, EXTENT // 4, LANES), WIRE),
        pltpu.VMEM((3, 2, 2, EDGE, LANES), WIRE),
        pltpu.VMEM((4, 8, LANES), f32),
        pltpu.VMEM((2, 8, LANES), f32),
        pltpu.VMEM((ty_size - 1, 8, LANES), f32),
        pltpu.VMEM((tx_size - 1, 8, LANES), f32),
        dma((2, tx_size)),
        dma((2, tx_size)),
        dma,
        dma((2, 3, len(SIDES))),
        dma((2, ty_size - 1)),
        dma((2, tx_size - 1)),
    ]
    return pl.pallas_call(
        functools.partial(whole_kernel, (ty_size, tx_size)),
        out_shape=(jax.ShapeDtypeStruct((TILE, TILE), f32), jax.ShapeDtypeStruct((TILE, TILE), f32)),
        in_specs=[vmem, vmem, smem, smem, smem],
        out_specs=(vmem, vmem),
        scratch_shapes=scratch,
        compiler_params=pltpu.CompilerParams(collective_id=0, has_side_effects=True),
        name="whole",
    )(exposures, point_spread, warp_steps, column[:, 0], block_cell)


def solution(mesh):
    placed = (
        P(("ty", "tx"), None, None),
        P(("ty", "tx"), None, None),
        P(("ty", "tx"), None),
        P(("ty", "tx"), None),
        P(("ty", "tx")),
    )
    return jax.shard_map(
        body, mesh=mesh, in_specs=placed, out_specs=(P("ty", "tx"), P("ty", "tx")), check_vma=False
    )
```

```python
import functools

import jax
import jax.numpy as jnp
from jax import lax
from jax.experimental import pallas as pl
from jax.experimental.pallas import tpu as pltpu
from jax.sharding import PartitionSpec as P

TILE = 512
SUB = 4
LANES = 128
GROUP = 32
MARGIN = 16
CAP = 2
EDGE = 2 * MARGIN
EXTENT = TILE + EDGE
PATCH = LANES + EDGE
ROWS = 144
PAD = 16
WIRE = jnp.bfloat16
SIDES = ((-1, 0), (1, 0), (0, -1), (0, 1), (-1, -1), (-1, 1), (1, -1), (1, 1))

damping = 0.05


def turn(value, shift):
    return pltpu.roll(value, shift % LANES, 1) if shift % LANES else value


def lanes_of(shape):
    return lax.broadcasted_iota(jnp.int32, shape, len(shape) - 1)


def pick_groups(parts):
    groups = lanes_of(parts[0].shape) >> 5
    value = parts[-1]
    for number in range(len(parts) - 2, -1, -1):
        value = jnp.where(groups == number, parts[number], value)
    return value


def make_taps(spread_ref, warp_ref, held_ref, taps_ref):
    side, frames = spread_ref.shape[:2]
    shape = (frames, LANES)
    index = lax.broadcasted_iota(jnp.int32, shape, 0)
    steps = [jnp.zeros(shape, jnp.int32), jnp.zeros(shape, jnp.int32)]
    for which in range(2):
        for frame in range(frames):
            steps[which] = jnp.where(index == frame, warp_ref[which, frame], steps[which])
    row_frac, col_frac = (step.astype(jnp.float32) / SUB for step in steps)
    held_ref[...] = jnp.zeros_like(held_ref)
    held_ref[:side, :frames, :side] = spread_ref[...]
    points = [held_ref[a, :frames] for a in range(side)]
    total = points[0]
    for point in points[1:]:
        total = total + point
    total = jnp.sum(total, axis=1, keepdims=True)
    points = [point / total for point in points] + [jnp.zeros(shape, jnp.float32)]
    points = [(1.0 - col_frac) * point + col_frac * turn(point, 1) for point in points]
    kernel = [(1.0 - row_frac) * points[0]]
    for a in range(1, side + 1):
        kernel.append((1.0 - row_frac) * points[a] + row_frac * points[a - 1])
    for row in range(16):
        a = row // 4 * 8 + row % 4
        held_ref[row, :frames] = kernel[a] + turn(kernel[a + 4], 64)
    for frame in range(frames):
        rows = [held_ref[row, frame : frame + 1] for row in range(16)]
        taps_ref[frame] = jnp.concatenate(rows, axis=0).astype(jnp.bfloat16)


def toeplitz(rows):
    tiles = []
    for j in range(8):
        halves = []
        for half in range(2):
            row = rows[8 * half + j : 8 * half + j + 1]
            spread = jnp.broadcast_to(row, (GROUP, LANES))
            halves.append(pltpu.roll(spread, 0, 1, stride=1, stride_axis=0))
        tiles.append(jnp.concatenate(halves, axis=1))
    return jnp.concatenate(tiles, axis=0).astype(jnp.bfloat16)


def blur(shifted_ref, first, matrix, joined_ref):
    for g in range(4):
        near = shifted_ref[first + g, :ROWS]
        far = shifted_ref[first + g, PATCH - ROWS :]
        product = lax.dot_general(
            jnp.concatenate([near, far], axis=1),
            matrix,
            (((1,), (1,)), ((), ())),
            preferred_element_type=jnp.float32,
        )
        joined_ref[g] = product[: ROWS - 8, :LANES] + product[8:, LANES:]
    total = None
    for step in range(4):
        chosen = pick_groups([joined_ref[(j + step) % 4, j : j + LANES] for j in range(4)])
        chosen = turn(chosen, 32 * step)
        total = chosen if total is None else total + chosen
    return total


def hold_turns(image, turned_ref):
    for step in range(4):
        turned_ref[step, PAD : PAD + LANES] = turn(image, 32 * step)


def blur_back(turned_ref, matrix, behind_ref):
    low = lanes_of((PATCH, LANES)) < 64
    folded = []
    for h in range(4):
        rows = pick_groups(
            [turned_ref[(j - h) % 4, PAD - 8 - j : PAD - 8 - j + ROWS + 8] for j in range(4)]
        )
        stacked = jnp.concatenate(
            [rows[8:].astype(jnp.bfloat16), rows[:ROWS].astype(jnp.bfloat16)], axis=1
        )
        product = jnp.dot(stacked, matrix, preferred_element_type=jnp.float32)
        near, far = product[:, :LANES], product[:, LANES:]
        folded.append(jnp.concatenate([near[:16], near[16:] + far[: ROWS - 16], far[ROWS - 16 :]], axis=0))
    sums = []
    for number in range(2):
        one, two = folded[number], folded[number + 2]
        behind_ref[number, 8 : 8 + PATCH] = jnp.where(low, turn(one, 64), two)
        ahead = jnp.where(low, one, turn(two, 64))
        sums.append(ahead + behind_ref[number, 4 : 4 + PATCH])
    moved = turn(sums[1], 32)
    wrapped = lanes_of(moved.shape) < GROUP
    return sums[0] + jnp.where(wrapped, 0.0, moved), jnp.where(wrapped, moved, 0.0)


def assemble(running_ref, index_ref, per_row, field_ref):
    block = LANES

    def part(row, col, side, first, count):
        if 0 <= row < per_row and 0 <= col < per_row:
            return [running_ref[index_ref[row * per_row + col], side, first : first + count]]
        return []

    for row in range(per_row + 1):
        for col in range(per_row + 1):
            both = part(row - 1, col, 0, block, EDGE) + part(row - 1, col - 1, 1, block, EDGE)
            rest = part(row, col, 0, 0, EDGE) + part(row, col - 1, 1, 0, EDGE)
            field_ref[col, row * block : row * block + EDGE] = sum((both + rest)[1:], (both + rest)[0])
            if row < per_row:
                count = block - EDGE
                body = part(row, col, 0, EDGE, count) + part(row, col - 1, 1, EDGE, count)
                field_ref[col, row * block + EDGE : (row + 1) * block] = sum(body[1:], body[0])


def flat_strip(strip_ref, tile):
    height = EXTENT // 4
    parts = [turn(strip_ref[tile, k * height : (k + 1) * height], 32 * k) for k in range(4)]
    return pick_groups(parts).astype(WIRE)


def add_flat(field_ref, tile, flat):
    height = EXTENT // 4
    wrapped = lanes_of((height, LANES)) < GROUP
    flat = flat.astype(jnp.float32)
    for k in range(4):
        rows = slice(k * height, (k + 1) * height)
        field_ref[tile, rows] += jnp.where(wrapped, turn(flat, -32 * k), 0.0)


def shift_field(field_ref, shifted_ref, per_row, sums_ref, row):
    chunk = 16

    tall = PATCH // chunk

    @pl.loop(0, per_row * tall)
    def _(step):
        number = step // tall * (LANES // chunk) + lax.rem(step, tall)
        start = pl.multiple_of(number * chunk, chunk)
        local = pl.multiple_of(lax.rem(step, tall) * chunk, chunk)
        cell = step // tall * per_row
        lanes = lanes_of((chunk, LANES))
        low, middle = lanes < 64, (lanes >= 32) & (lanes < 96)
        now = [field_ref[col, pl.ds(start, chunk)] for col in range(per_row + 1)]
        later = [field_ref[col, pl.ds(start + 4, chunk)] for col in range(per_row + 1)]
        by96 = [turn(jnp.where(middle, a, b), 96) for a, b in zip(now, later)]
        by32 = [turn(jnp.where(middle, b, a), 32) for a, b in zip(now, later)]
        for col in range(per_row):
            a, b = now[col], later[col]
            by64 = turn(jnp.where(low, b, a), 64)
            parts = [
                jnp.where(low, a, by64),
                jnp.where(low, by96[col], by32[col]),
                jnp.where(low, by64, b),
                pick_groups([by32[col], by32[col + 1], by96[col], by96[col + 1]]),
            ]
            for g in range(4):
                shifted_ref[4 * (cell + col) + g, pl.ds(local, chunk)] = parts[g].astype(jnp.bfloat16)
        squares = None
        for col in range(per_row + 1):
            value = now[col]
            if col == 0:
                value = jnp.where(lanes < MARGIN, 0.0, value)
            if col == per_row:
                value = jnp.where(lanes < MARGIN, value, 0.0)
            squares = value * value if squares is None else squares + value * value
        once = (lax.rem(step, tall) < LANES // chunk) | (cell == per_row * (per_row - 1))
        place = start + lax.broadcasted_iota(jnp.int32, squares.shape, 0)
        squares = jnp.where((place >= MARGIN) & (place < EXTENT - MARGIN), squares, 0.0)
        squares = squares.reshape(chunk // 8, 8, LANES).sum(axis=0)
        sums_ref[row] += jnp.where(once, squares, 0.0)


def whole_kernel(
    sizes,
    exposures_ref,
    spread_ref,
    warp_ref,
    column_ref,
    cell_ref,
    solution_ref,
    residual_ref,
    pad_ref,
    taps_ref,
    send_ref,
    frames_ref,
    tag_send_ref,
    tags_ref,
    tag_smem,
    key_smem,
    order_smem,
    index_smem,
    matrix_ref,
    patch_ref,
    running_ref,
    turned_ref,
    behind_ref,
    joined_ref,
    shifted_ref,
    field_ref,
    row_send_ref,
    col_send_ref,
    row_land_ref,
    col_land_ref,
    corner_land_ref,
    sums_ref,
    total_ref,
    total_land_ref,
    tag_sems,
    frame_sems,
    local_sem,
    halo_sems,
    sum_sems,
):
    ty_size, tx_size = sizes
    frame_count, block = exposures_ref.shape[:2]
    per_row = TILE // block
    cells = per_row * per_row
    slots = CAP * tx_size
    ty, tx = lax.axis_index("ty"), lax.axis_index("tx")

    def has(side):
        row, col = side
        ok = None
        for step, place, size in ((row, ty, ty_size), (col, tx, tx_size)):
            test = (place > 0) if step < 0 else (place < size - 1) if step > 0 else None
            if test is not None:
                ok = test if ok is None else ok & test
        return ok

    def at(side):
        return {"ty": ty + side[0], "tx": tx + side[1]}

    barrier = pltpu.get_barrier_semaphore()

    def greet(device):
        pl.semaphore_signal(barrier, inc=1, device_id=device, device_id_type=pl.DeviceIdType.MESH)

    @pl.loop(1, ty_size * tx_size)
    def _(step):
        peer = lax.rem(ty * tx_size + tx + step, ty_size * tx_size)
        greet({"ty": peer // tx_size, "tx": lax.rem(peer, tx_size)})

    make_taps(spread_ref, warp_ref, pad_ref, taps_ref)

    running_ref[0] = jnp.zeros(running_ref.shape[1:], jnp.float32)
    turned_ref[...] = jnp.zeros_like(turned_ref)
    behind_ref[...] = jnp.zeros_like(behind_ref)
    sums_ref[...] = jnp.zeros_like(sums_ref)
    for number in range(3):
        field_ref[number, :, EXTENT:] = jnp.zeros((per_row + 1, 8, LANES), jnp.float32)

    pl.semaphore_wait(barrier, ty_size * tx_size - 1)

    def sources(target):
        first, second, count = jnp.int32(0), jnp.int32(0), jnp.int32(0)
        for frame in range(frame_count):
            match = column_ref[frame_count - 1 - frame] == target
            first = jnp.where(match, frame_count - 1 - frame, first)
            second = jnp.where(column_ref[frame] == target, frame, second)
            count = count + jnp.where(match, 1, 0)
        return first, second, count

    def tag_copy(step):
        return pltpu.make_async_remote_copy(
            src_ref=tag_send_ref.at[step],
            dst_ref=tags_ref.at[step],
            send_sem=tag_sems.at[0, step],
            recv_sem=tag_sems.at[1, step],
            device_id={"tx": lax.rem(tx + step, tx_size)},
            device_id_type=pl.DeviceIdType.MESH,
        )

    def frame_copy(step):
        return pltpu.make_async_remote_copy(
            src_ref=send_ref.at[step],
            dst_ref=frames_ref.at[step],
            send_sem=frame_sems.at[0, step],
            recv_sem=frame_sems.at[1, step],
            device_id={"tx": lax.rem(tx + step, tx_size)},
            device_id_type=pl.DeviceIdType.MESH,
        )

    def tags_for(step):
        first, second, count = sources(lax.rem(tx + step, tx_size))
        one = jnp.where(count >= 1, cell_ref[first], -1)
        two = jnp.where(count >= 2, cell_ref[second], -1)
        shape = tags_ref.shape[1:]
        rows = lax.broadcasted_iota(jnp.int32, shape, 0)
        return jnp.where(rows == 0, jnp.full(shape, one, jnp.int32), jnp.full(shape, two, jnp.int32))

    def fill(ref, step):
        first, second, _ = sources(lax.rem(tx + step, tx_size))
        for number, origin in enumerate((first, second)):
            ref[step, number, :block] = exposures_ref[origin].astype(jnp.bfloat16)
            ref[step, number, block:] = taps_ref[origin]

    tags_ref[0] = tags_for(0)

    @pl.loop(1, tx_size)
    def _(step):
        tag_send_ref[step] = tags_for(step)
        tag_copy(step).start()

    @pl.loop(1, tx_size)
    def _(step):
        fill(send_ref, step)
        frame_copy(step).start()

    fill(frames_ref, 0)

    def first_pass(step):
        for number in range(CAP):
            slot = CAP * step + number
            matrix = toeplitz(frames_ref[step, number, block:].astype(jnp.float32))
            matrix_ref[slot] = matrix
            hold_turns(frames_ref[step, number, :block].astype(jnp.float32), turned_ref.at[number])
            left, right = blur_back(turned_ref.at[number], matrix, behind_ref.at[number])
            patch_ref[slot, 0] = left
            patch_ref[slot, 1] = right

    first_pass(0)

    @pl.loop(1, tx_size)
    def _(step):
        tag_copy(step).wait()

    local = pltpu.make_async_copy(tags_ref, tag_smem, local_sem)
    local.start()
    local.wait()

    @pl.loop(0, slots)
    def _(slot):
        key_smem[slot] = tag_smem[slot // CAP, lax.rem(slot, CAP), 0] * slots + slot

    @pl.loop(0, slots)
    def _(slot):
        key = key_smem[slot]
        rank = jnp.int32(0)
        for other in range(slots):
            rank = rank + jnp.where(key_smem[other] < key, 1, 0)
        order_smem[0, slot] = rank

    @pl.loop(0, slots)
    def _(place):
        slot = jnp.int32(0)
        for other in range(slots):
            slot = jnp.where(order_smem[0, other] == place, other, slot)
        order_smem[1, place] = slot
        cell = tag_smem[slot // CAP, lax.rem(slot, CAP), 0]
        order_smem[2, place] = cell

    @pl.loop(0, cells)
    def _(cell):
        upto, equal = jnp.int32(0), jnp.int32(0)
        for place in range(slots):
            value = order_smem[2, place]
            upto = upto + jnp.where(value <= cell, 1, 0)
            equal = equal + jnp.where(value == cell, 1, 0)
        index_smem[cell] = jnp.where(equal > 0, upto, 0)

    @pl.loop(1, tx_size)
    def _(step):
        frame_copy(step).wait()
        first_pass(step)

    def same(place):
        before = order_smem[2, jnp.maximum(place - 1, 0)]
        return (place > 0) & (before == order_smem[2, place])

    @pl.loop(0, slots)
    def _(place):
        kept = same(place)
        slot = order_smem[1, place]
        for side in range(2):
            running_ref[place + 1, side] = patch_ref[slot, side] + jnp.where(
                kept, running_ref[place, side], 0.0
            )

    def halo_copy(turn_number, which):
        row, col = SIDES[which]
        if col == 0:
            source = row_send_ref.at[turn_number, (row + 1) // 2]
            target = row_land_ref.at[turn_number, (1 - row) // 2]
        elif row == 0:
            source = col_send_ref.at[turn_number, (col + 1) // 2]
            target = col_land_ref.at[turn_number, (1 - col) // 2]
        else:
            source = row_send_ref.at[turn_number, (row + 1) // 2, per_row * ((col + 1) // 2)]
            target = corner_land_ref.at[turn_number, (1 - row) // 2, (1 - col) // 2]
        return pltpu.make_async_remote_copy(
            src_ref=source,
            dst_ref=target,
            send_sem=halo_sems.at[0, turn_number, which],
            recv_sem=halo_sems.at[1, turn_number, SIDES.index((-row, -col))],
            device_id=at(SIDES[which]),
            device_id_type=pl.DeviceIdType.MESH,
        )

    def share_edges(number):
        own = field_ref.at[number]
        for end in range(2):
            col_send_ref[number, end] = flat_strip(own, per_row * end)
        for which in (2, 3):
            pl.when(has(SIDES[which]))(lambda which=which: halo_copy(number, which).start())
        for end in range(2):
            for col in range(per_row + 1):
                row_send_ref[number, end, col] = own[col, TILE * end : TILE * end + EDGE].astype(WIRE)
        for which in (4, 5, 6, 7, 0, 1):
            pl.when(has(SIDES[which]))(lambda which=which: halo_copy(number, which).start())

    def take_edges(number):
        own = field_ref.at[number]

        def land(which):
            row, col = SIDES[which]
            halo_copy(number, which).wait_send()
            back = SIDES.index((row, col))
            pltpu.make_async_remote_copy(
                src_ref=halo_source(which),
                dst_ref=halo_target(which),
                send_sem=halo_sems.at[0, number, which],
                recv_sem=halo_sems.at[1, number, back],
                device_id=at(SIDES[which]),
                device_id_type=pl.DeviceIdType.MESH,
            ).wait_recv()
            if col == 0:
                end = (row + 1) // 2
                for tile in range(per_row + 1):
                    own[tile, TILE * end : TILE * end + EDGE] += row_land_ref[number, end, tile].astype(
                        jnp.float32
                    )
            elif row == 0:
                end = (col + 1) // 2
                add_flat(own, per_row * end, col_land_ref[number, end])
            else:
                end, tile = (row + 1) // 2, per_row * ((col + 1) // 2)
                value = corner_land_ref[number, end, (col + 1) // 2].astype(jnp.float32)
                inside = lanes_of(value.shape) < EDGE
                own[tile, TILE * end : TILE * end + EDGE] += jnp.where(inside, value, 0.0)

        def halo_source(which):
            row, col = SIDES[which]
            if col == 0:
                return row_send_ref.at[number, (row + 1) // 2]
            if row == 0:
                return col_send_ref.at[number, (col + 1) // 2]
            return row_send_ref.at[number, (row + 1) // 2, per_row * ((col + 1) // 2)]

        def halo_target(which):
            row, col = SIDES[which]
            if col == 0:
                return row_land_ref.at[number, (row + 1) // 2]
            if row == 0:
                return col_land_ref.at[number, (col + 1) // 2]
            return corner_land_ref.at[number, (row + 1) // 2, (col + 1) // 2]

        for which in range(len(SIDES)):
            pl.when(has(SIDES[which]))(functools.partial(land, which))

    def clear_outside(number):
        own = field_ref.at[number]

        @pl.when(ty == 0)
        def _():
            for tile in range(per_row + 1):
                own[tile, :MARGIN] = jnp.zeros((MARGIN, LANES), jnp.float32)

        @pl.when(ty == ty_size - 1)
        def _():
            for tile in range(per_row + 1):
                own[tile, TILE + MARGIN : EXTENT] = jnp.zeros((MARGIN, LANES), jnp.float32)

        @pl.when(tx == 0)
        def _():
            value = own[0, :EXTENT]
            own[0, :EXTENT] = jnp.where(lanes_of(value.shape) < MARGIN, 0.0, value)

        @pl.when(tx == tx_size - 1)
        def _():
            value = own[per_row, :EXTENT]
            own[per_row, :EXTENT] = jnp.where(lanes_of(value.shape) < MARGIN, value, 0.0)

    def gather_field(number):
        assemble(running_ref, index_smem, per_row, field_ref.at[number])
        share_edges(number)

    def damp(number):
        for tile in range(per_row + 1):
            field_ref[number, tile, :EXTENT] += damping * field_ref[number - 1, tile, :EXTENT]

    def forward(row, place, lane):
        cell = order_smem[2, place]
        matrix = matrix_ref[order_smem[1, place]]
        modelled = blur(shifted_ref, jnp.maximum(cell, 0) * 4, matrix, joined_ref.at[lane])
        squares = modelled * modelled
        squares = squares.reshape(block // 8, 8, LANES).sum(axis=0)
        sums_ref[row] += jnp.where(cell >= 0, squares, 0.0)
        hold_turns(modelled.astype(jnp.bfloat16).astype(jnp.float32), turned_ref.at[lane])

    def backward(place, lane):
        kept = same(place)
        matrix = matrix_ref[order_smem[1, place]]
        left, right = blur_back(turned_ref.at[lane], matrix, behind_ref.at[lane])
        running_ref[place + 1, 0] = left + jnp.where(kept, running_ref[place, 0], 0.0)
        running_ref[place + 1, 1] = right + jnp.where(kept, running_ref[place, 1], 0.0)

    def normal_pass(row, between):
        for lane in range(CAP):
            forward(row, lane, lane)

        @pl.loop(1, slots // CAP)
        def _(step):
            for lane in range(CAP):
                backward(CAP * (step - 1) + lane, lane)
            for lane in range(CAP):
                forward(row, CAP * step + lane, lane)

        between()
        for lane in range(CAP):
            backward(slots - CAP + lane, lane)

    gather_field(0)
    take_edges(0)
    clear_outside(0)
    shift_field(field_ref.at[0], shifted_ref, per_row, sums_ref, 0)
    normal_pass(1, lambda: None)
    gather_field(1)
    take_edges(1)
    clear_outside(1)
    damp(1)
    shift_field(field_ref.at[1], shifted_ref, per_row, sums_ref, 2)
    def sum_copy(step):
        peer = lax.rem(ty * tx_size + tx + step, ty_size * tx_size)
        return pltpu.make_async_remote_copy(
            src_ref=total_ref,
            dst_ref=total_land_ref.at[step],
            send_sem=sum_sems.at[0, step],
            recv_sem=sum_sems.at[1, step],
            device_id={"ty": peer // tx_size, "tx": lax.rem(peer, tx_size)},
            device_id_type=pl.DeviceIdType.MESH,
        )

    def send_sums():
        packed = jnp.zeros((1, LANES), jnp.float32)
        for number in range(4):
            value = jnp.sum(sums_ref[number], axis=0, keepdims=True)
            value = jnp.sum(value, axis=1, keepdims=True)
            packed = jnp.where(lanes_of(packed.shape) == number, value, packed)
        total_ref[...] = packed
        total_land_ref[0] = packed

        @pl.loop(1, ty_size * tx_size)
        def _(step):
            sum_copy(step).start()

    normal_pass(3, send_sums)
    gather_field(2)
    take_edges(2)
    damp(2)

    @pl.loop(1, ty_size * tx_size)
    def _(step):
        sum_copy(step).wait()

    total = total_land_ref[0]
    for step in range(1, ty_size * tx_size):
        total = total + total_land_ref[step]
    wide = jnp.zeros((1, LANES), jnp.float32)
    sums = [
        wide + jnp.sum(jnp.where(lanes_of(wide.shape) == number, total, 0.0), axis=1, keepdims=True)
        for number in range(4)
    ]
    r00 = sums[0]
    r01 = sums[1] + damping * r00
    r11 = sums[2]
    r12 = sums[3] + damping * r11
    step0 = r00 / r01
    norm_next = r00 - 2.0 * step0 * r01 + step0 * step0 * r11
    grown = 1.0 + norm_next / r00
    curvature = grown * grown * r01 - 2.0 * grown * step0 * r11 + step0 * step0 * r12
    step1 = norm_next / curvature
    x0 = step0 + step1 * grown
    x1 = -step1 * step0
    y1 = -step0 - step1 * grown
    y2 = step1 * step0

    chunk = 32

    @pl.loop(0, TILE // chunk)
    def _(number):
        start = pl.multiple_of(number * chunk, chunk)
        source = pl.ds(pl.multiple_of(start + MARGIN, 8), chunk)
        inside = lanes_of((chunk, LANES)) < LANES - MARGIN
        solved, left = [], []
        for tile in range(per_row + 1):
            q0, q1, q2 = (field_ref[k, tile, source] for k in range(3))
            solved.append(turn(x0 * q0 + x1 * q1, -MARGIN))
            left.append(turn(q0 + y1 * q1 + y2 * q2, -MARGIN))
        for tile in range(per_row):
            lanes = slice(tile * LANES, (tile + 1) * LANES)
            solution_ref[pl.ds(start, chunk), lanes] = jnp.where(inside, solved[tile], solved[tile + 1])
            residual_ref[pl.ds(start, chunk), lanes] = jnp.where(inside, left[tile], left[tile + 1])


def body(exposures, point_spread, warp_steps, column, block_cell):
    ty_size, tx_size = lax.axis_size("ty"), lax.axis_size("tx")
    frame_count, block = exposures.shape[:2]
    per_row = TILE // block
    slots = CAP * tx_size
    tall = EXTENT + 8
    f32, bf16 = jnp.float32, jnp.bfloat16
    vmem = pl.BlockSpec(memory_space=pltpu.VMEM)
    smem = pl.BlockSpec(memory_space=pltpu.SMEM)
    dma = pltpu.SemaphoreType.DMA
    scratch = [
        pltpu.VMEM((GROUP, frame_count, LANES), f32),
        pltpu.VMEM((frame_count, 16, LANES), bf16),
        pltpu.VMEM((tx_size, CAP, ROWS, LANES), bf16),
        pltpu.VMEM((tx_size, CAP, ROWS, LANES), bf16),
        pltpu.VMEM((tx_size, 8, LANES), jnp.int32),
        pltpu.VMEM((tx_size, 8, LANES), jnp.int32),
        pltpu.SMEM((tx_size, 8, LANES), jnp.int32),
        pltpu.SMEM((slots,), jnp.int32),
        pltpu.SMEM((3, slots), jnp.int32),
        pltpu.SMEM((per_row * per_row,), jnp.int32),
        pltpu.VMEM((slots, 256, 256), bf16),
        pltpu.VMEM((slots, 2, PATCH, LANES), f32),
        pltpu.VMEM((slots + 1, 2, PATCH, LANES), f32),
        pltpu.VMEM((CAP, 4, PAD + ROWS, LANES), f32),
        pltpu.VMEM((CAP, 2, 8 + PATCH, LANES), f32),
        pltpu.VMEM((CAP, 4, ROWS - 8, LANES), f32),
        pltpu.VMEM((4 * per_row * per_row, PATCH, LANES), bf16),
        pltpu.VMEM((3, per_row + 1, tall, LANES), f32),
        pltpu.VMEM((3, 2, per_row + 1, EDGE, LANES), WIRE),
        pltpu.VMEM((3, 2, EXTENT // 4, LANES), WIRE),
        pltpu.VMEM((3, 2, per_row + 1, EDGE, LANES), WIRE),
        pltpu.VMEM((3, 2, EXTENT // 4, LANES), WIRE),
        pltpu.VMEM((3, 2, 2, EDGE, LANES), WIRE),
        pltpu.VMEM((4, 8, LANES), f32),
        pltpu.VMEM((1, LANES), f32),
        pltpu.VMEM((ty_size * tx_size, 1, LANES), f32),
        dma((2, tx_size)),
        dma((2, tx_size)),
        dma,
        dma((2, 3, len(SIDES))),
        dma((2, ty_size * tx_size)),
    ]
    return pl.pallas_call(
        functools.partial(whole_kernel, (ty_size, tx_size)),
        out_shape=(jax.ShapeDtypeStruct((TILE, TILE), f32), jax.ShapeDtypeStruct((TILE, TILE), f32)),
        in_specs=[vmem, vmem, smem, smem, smem],
        out_specs=(vmem, vmem),
        scratch_shapes=scratch,
        compiler_params=pltpu.CompilerParams(
            collective_id=0, has_side_effects=True, vmem_limit_bytes=36 * 1024 * 1024
        ),
        name="whole",
    )(exposures, point_spread.transpose(1, 0, 2), warp_steps.T, column[:, 0], block_cell)


def solution(mesh):
    placed = (
        P(("ty", "tx"), None, None),
        P(("ty", "tx"), None, None),
        P(("ty", "tx"), None),
        P(("ty", "tx"), None),
        P(("ty", "tx")),
    )
    return jax.shard_map(
        body, mesh=mesh, in_specs=placed, out_specs=(P("ty", "tx"), P("ty", "tx")), check_vma=False
    )
```

```python
import functools

import jax
import jax.numpy as jnp
from jax import lax
from jax.experimental import pallas as pl
from jax.experimental.pallas import tpu as pltpu
from jax.sharding import PartitionSpec as P

TILE = 512
SUB = 4
LANES = 128
GROUP = 32
MARGIN = 16
CAP = 2
EDGE = 2 * MARGIN
EXTENT = TILE + EDGE
PATCH = LANES + EDGE
ROWS = 144
PAD = 16
WIRE = jnp.bfloat16
SIDES = ((-1, 0), (1, 0), (0, -1), (0, 1), (-1, -1), (-1, 1), (1, -1), (1, 1))

damping = 0.05


def turn(value, shift):
    return pltpu.roll(value, shift % LANES, 1) if shift % LANES else value


def lanes_of(shape):
    return lax.broadcasted_iota(jnp.int32, shape, len(shape) - 1)


def pick_groups(parts):
    groups = lanes_of(parts[0].shape) >> 5
    value = parts[-1]
    for number in range(len(parts) - 2, -1, -1):
        value = jnp.where(groups == number, parts[number], value)
    return value


def make_taps(spread_ref, warp_ref, held_ref, taps_ref):
    side, frames = spread_ref.shape[:2]
    shape = (frames, LANES)
    index = lax.broadcasted_iota(jnp.int32, shape, 0)
    steps = [jnp.zeros(shape, jnp.int32), jnp.zeros(shape, jnp.int32)]
    for which in range(2):
        for frame in range(frames):
            steps[which] = jnp.where(index == frame, warp_ref[which, frame], steps[which])
    row_frac, col_frac = (step.astype(jnp.float32) / SUB for step in steps)
    held_ref[...] = jnp.zeros_like(held_ref)
    held_ref[:side, :frames, :side] = spread_ref[...]
    points = [held_ref[a, :frames] for a in range(side)]
    total = points[0]
    for point in points[1:]:
        total = total + point
    total = jnp.sum(total, axis=1, keepdims=True)
    points = [point / total for point in points] + [jnp.zeros(shape, jnp.float32)]
    points = [(1.0 - col_frac) * point + col_frac * turn(point, 1) for point in points]
    kernel = [(1.0 - row_frac) * points[0]]
    for a in range(1, side + 1):
        kernel.append((1.0 - row_frac) * points[a] + row_frac * points[a - 1])
    for row in range(16):
        a = row // 4 * 8 + row % 4
        held_ref[row, :frames] = kernel[a] + turn(kernel[a + 4], 64)
    for frame in range(frames):
        rows = [held_ref[row, frame : frame + 1] for row in range(16)]
        taps_ref[frame] = jnp.concatenate(rows, axis=0).astype(jnp.bfloat16)


def toeplitz(rows):
    tiles = []
    for j in range(8):
        halves = []
        for half in range(2):
            row = rows[8 * half + j : 8 * half + j + 1]
            spread = jnp.broadcast_to(row, (GROUP, LANES))
            halves.append(pltpu.roll(spread, 0, 1, stride=1, stride_axis=0))
        tiles.append(jnp.concatenate(halves, axis=1))
    return jnp.concatenate(tiles, axis=0).astype(jnp.bfloat16)


def blur(shifted_ref, first, matrix, joined_ref):
    for g in range(4):
        near = shifted_ref[first + g, :ROWS]
        far = shifted_ref[first + g, PATCH - ROWS :]
        product = lax.dot_general(
            jnp.concatenate([near, far], axis=1),
            matrix,
            (((1,), (1,)), ((), ())),
            preferred_element_type=jnp.float32,
        )
        joined_ref[g] = product[: ROWS - 8, :LANES] + product[8:, LANES:]
    total = None
    for step in range(4):
        chosen = pick_groups([joined_ref[(j + step) % 4, j : j + LANES] for j in range(4)])
        chosen = turn(chosen, 32 * step)
        total = chosen if total is None else total + chosen
    return total


def hold_turns(image, turned_ref):
    for step in range(4):
        turned_ref[step, PAD : PAD + LANES] = turn(image, 32 * step)


def blur_back(turned_ref, matrix, behind_ref):
    low = lanes_of((PATCH, LANES)) < 64
    folded = []
    for h in range(4):
        rows = pick_groups(
            [turned_ref[(j - h) % 4, PAD - 8 - j : PAD - 8 - j + ROWS + 8] for j in range(4)]
        )
        stacked = jnp.concatenate(
            [rows[8:].astype(jnp.bfloat16), rows[:ROWS].astype(jnp.bfloat16)], axis=1
        )
        product = jnp.dot(stacked, matrix, preferred_element_type=jnp.float32)
        near, far = product[:, :LANES], product[:, LANES:]
        folded.append(jnp.concatenate([near[:16], near[16:] + far[: ROWS - 16], far[ROWS - 16 :]], axis=0))
    sums = []
    for number in range(2):
        one, two = folded[number], folded[number + 2]
        behind_ref[number, 8 : 8 + PATCH] = jnp.where(low, turn(one, 64), two)
        ahead = jnp.where(low, one, turn(two, 64))
        sums.append(ahead + behind_ref[number, 4 : 4 + PATCH])
    moved = turn(sums[1], 32)
    wrapped = lanes_of(moved.shape) < GROUP
    return sums[0] + jnp.where(wrapped, 0.0, moved), jnp.where(wrapped, moved, 0.0)


def assemble(running_ref, index_ref, per_row, field_ref):
    block = LANES

    def part(row, col, side, first, count):
        if 0 <= row < per_row and 0 <= col < per_row:
            return [running_ref[index_ref[row * per_row + col], side, first : first + count]]
        return []

    for row in range(per_row + 1):
        for col in range(per_row + 1):
            both = part(row - 1, col, 0, block, EDGE) + part(row - 1, col - 1, 1, block, EDGE)
            rest = part(row, col, 0, 0, EDGE) + part(row, col - 1, 1, 0, EDGE)
            field_ref[col, row * block : row * block + EDGE] = sum((both + rest)[1:], (both + rest)[0])
            if row < per_row:
                count = block - EDGE
                body = part(row, col, 0, EDGE, count) + part(row, col - 1, 1, EDGE, count)
                field_ref[col, row * block + EDGE : (row + 1) * block] = sum(body[1:], body[0])


def flat_strip(strip_ref, tile):
    height = EXTENT // 4
    parts = [turn(strip_ref[tile, k * height : (k + 1) * height], 32 * k) for k in range(4)]
    return pick_groups(parts).astype(WIRE)


def add_flat(field_ref, tile, flat):
    height = EXTENT // 4
    wrapped = lanes_of((height, LANES)) < GROUP
    flat = flat.astype(jnp.float32)
    for k in range(4):
        rows = slice(k * height, (k + 1) * height)
        field_ref[tile, rows] += jnp.where(wrapped, turn(flat, -32 * k), 0.0)


def shift_field(field_ref, shifted_ref, per_row, sums_ref, row):
    chunk = PATCH // 2

    tall = PATCH // chunk

    @pl.loop(0, per_row * tall)
    def _(step):
        local = pl.multiple_of(lax.rem(step, tall) * chunk, 16)
        start = pl.multiple_of(step // tall * LANES + local, 16)
        cell = step // tall * per_row
        lanes = lanes_of((chunk, LANES))
        low, middle = lanes < 64, (lanes >= 32) & (lanes < 96)
        now = [field_ref[col, pl.ds(start, chunk)] for col in range(per_row + 1)]
        later = [field_ref[col, pl.ds(start + 4, chunk)] for col in range(per_row + 1)]
        by96 = [turn(jnp.where(middle, a, b), 96) for a, b in zip(now, later)]
        by32 = [turn(jnp.where(middle, b, a), 32) for a, b in zip(now, later)]
        for col in range(per_row):
            a, b = now[col], later[col]
            by64 = turn(jnp.where(low, b, a), 64)
            parts = [
                jnp.where(low, a, by64),
                jnp.where(low, by96[col], by32[col]),
                jnp.where(low, by64, b),
                pick_groups([by32[col], by32[col + 1], by96[col], by96[col + 1]]),
            ]
            for g in range(4):
                shifted_ref[4 * (cell + col) + g, pl.ds(local, chunk)] = parts[g].astype(jnp.bfloat16)
        squares = None
        for col in range(per_row + 1):
            value = now[col]
            if col == 0:
                value = jnp.where(lanes < MARGIN, 0.0, value)
            if col == per_row:
                value = jnp.where(lanes < MARGIN, value, 0.0)
            squares = value * value if squares is None else squares + value * value
        place = lax.broadcasted_iota(jnp.int32, squares.shape, 0)
        last = jnp.where(cell == per_row * (per_row - 1), LANES, 0)
        inside = (place + start >= MARGIN) & (place + start < EXTENT - MARGIN)
        squares = jnp.where(inside & (place + local < LANES + last), squares, 0.0)
        sums_ref[row] += squares.reshape(chunk // 8, 8, LANES).sum(axis=0)


def whole_kernel(
    sizes,
    exposures_ref,
    spread_ref,
    warp_ref,
    column_ref,
    cell_ref,
    solution_ref,
    residual_ref,
    pad_ref,
    taps_ref,
    send_ref,
    frames_ref,
    tag_send_ref,
    tags_ref,
    tag_smem,
    key_smem,
    order_smem,
    index_smem,
    matrix_ref,
    patch_ref,
    running_ref,
    turned_ref,
    behind_ref,
    joined_ref,
    shifted_ref,
    field_ref,
    row_send_ref,
    col_send_ref,
    row_land_ref,
    col_land_ref,
    corner_land_ref,
    sums_ref,
    total_ref,
    total_land_ref,
    tag_sems,
    frame_sems,
    local_sem,
    halo_sems,
    sum_sems,
):
    ty_size, tx_size = sizes
    frame_count, block = exposures_ref.shape[:2]
    per_row = TILE // block
    cells = per_row * per_row
    slots = CAP * tx_size
    ty, tx = lax.axis_index("ty"), lax.axis_index("tx")

    def has(side):
        row, col = side
        ok = None
        for step, place, size in ((row, ty, ty_size), (col, tx, tx_size)):
            test = (place > 0) if step < 0 else (place < size - 1) if step > 0 else None
            if test is not None:
                ok = test if ok is None else ok & test
        return ok

    def at(side):
        return {"ty": ty + side[0], "tx": tx + side[1]}

    barrier = pltpu.get_barrier_semaphore()

    def greet(device):
        pl.semaphore_signal(barrier, inc=1, device_id=device, device_id_type=pl.DeviceIdType.MESH)

    @pl.loop(1, ty_size * tx_size)
    def _(step):
        peer = lax.rem(ty * tx_size + tx + step, ty_size * tx_size)
        greet({"ty": peer // tx_size, "tx": lax.rem(peer, tx_size)})

    make_taps(spread_ref, warp_ref, pad_ref, taps_ref)

    running_ref[0] = jnp.zeros(running_ref.shape[1:], jnp.float32)
    turned_ref[...] = jnp.zeros_like(turned_ref)
    behind_ref[...] = jnp.zeros_like(behind_ref)
    sums_ref[...] = jnp.zeros_like(sums_ref)
    for number in range(3):
        field_ref[number, :, EXTENT:] = jnp.zeros((per_row + 1, 8, LANES), jnp.float32)

    pl.semaphore_wait(barrier, ty_size * tx_size - 1)

    def sources(target):
        first, second, count = jnp.int32(0), jnp.int32(0), jnp.int32(0)
        for frame in range(frame_count):
            match = column_ref[frame_count - 1 - frame] == target
            first = jnp.where(match, frame_count - 1 - frame, first)
            second = jnp.where(column_ref[frame] == target, frame, second)
            count = count + jnp.where(match, 1, 0)
        return first, second, count

    def tag_copy(step):
        return pltpu.make_async_remote_copy(
            src_ref=tag_send_ref.at[step],
            dst_ref=tags_ref.at[step],
            send_sem=tag_sems.at[0, step],
            recv_sem=tag_sems.at[1, step],
            device_id={"tx": lax.rem(tx + step, tx_size)},
            device_id_type=pl.DeviceIdType.MESH,
        )

    def frame_copy(step):
        return pltpu.make_async_remote_copy(
            src_ref=send_ref.at[step],
            dst_ref=frames_ref.at[step],
            send_sem=frame_sems.at[0, step],
            recv_sem=frame_sems.at[1, step],
            device_id={"tx": lax.rem(tx + step, tx_size)},
            device_id_type=pl.DeviceIdType.MESH,
        )

    def tags_for(step):
        first, second, count = sources(lax.rem(tx + step, tx_size))
        one = jnp.where(count >= 1, cell_ref[first], -1)
        two = jnp.where(count >= 2, cell_ref[second], -1)
        shape = tags_ref.shape[1:]
        rows = lax.broadcasted_iota(jnp.int32, shape, 0)
        return jnp.where(rows == 0, jnp.full(shape, one, jnp.int32), jnp.full(shape, two, jnp.int32))

    def fill(ref, step):
        first, second, _ = sources(lax.rem(tx + step, tx_size))
        for number, origin in enumerate((first, second)):
            ref[step, number, :block] = exposures_ref[origin].astype(jnp.bfloat16)
            ref[step, number, block:] = taps_ref[origin]

    tags_ref[0] = tags_for(0)

    @pl.loop(1, tx_size, unroll=True)
    def _(step):
        tag_send_ref[step] = tags_for(step)
        tag_copy(step).start()

    @pl.loop(1, tx_size, unroll=True)
    def _(step):
        fill(send_ref, step)
        frame_copy(step).start()

    fill(frames_ref, 0)

    def first_pass(step):
        for number in range(CAP):
            slot = CAP * step + number
            matrix = toeplitz(frames_ref[step, number, block:].astype(jnp.float32))
            matrix_ref[slot] = matrix
            hold_turns(frames_ref[step, number, :block].astype(jnp.float32), turned_ref.at[number])
            left, right = blur_back(turned_ref.at[number], matrix, behind_ref.at[number])
            patch_ref[slot, 0] = left
            patch_ref[slot, 1] = right

    first_pass(0)

    @pl.loop(1, tx_size, unroll=True)
    def _(step):
        tag_copy(step).wait()

    local = pltpu.make_async_copy(tags_ref, tag_smem, local_sem)
    local.start()
    local.wait()

    @pl.loop(0, slots)
    def _(slot):
        key_smem[slot] = tag_smem[slot // CAP, lax.rem(slot, CAP), 0] * slots + slot

    @pl.loop(0, slots)
    def _(slot):
        key = key_smem[slot]
        rank = jnp.int32(0)
        for other in range(slots):
            rank = rank + jnp.where(key_smem[other] < key, 1, 0)
        order_smem[0, slot] = rank

    @pl.loop(0, slots)
    def _(place):
        slot = jnp.int32(0)
        for other in range(slots):
            slot = jnp.where(order_smem[0, other] == place, other, slot)
        order_smem[1, place] = slot
        cell = tag_smem[slot // CAP, lax.rem(slot, CAP), 0]
        order_smem[2, place] = cell

    @pl.loop(0, cells)
    def _(cell):
        upto, equal = jnp.int32(0), jnp.int32(0)
        for place in range(slots):
            value = order_smem[2, place]
            upto = upto + jnp.where(value <= cell, 1, 0)
            equal = equal + jnp.where(value == cell, 1, 0)
        index_smem[cell] = jnp.where(equal > 0, upto, 0)

    @pl.loop(1, tx_size)
    def _(step):
        frame_copy(step).wait()
        first_pass(step)

    def same(place):
        before = order_smem[2, jnp.maximum(place - 1, 0)]
        return (place > 0) & (before == order_smem[2, place])

    @pl.loop(0, slots, unroll=4)
    def _(place):
        kept = same(place)
        slot = order_smem[1, place]
        for side in range(2):
            running_ref[place + 1, side] = patch_ref[slot, side] + jnp.where(
                kept, running_ref[place, side], 0.0
            )

    def halo_copy(turn_number, which):
        row, col = SIDES[which]
        if col == 0:
            source = row_send_ref.at[turn_number, (row + 1) // 2]
            target = row_land_ref.at[turn_number, (1 - row) // 2]
        elif row == 0:
            source = col_send_ref.at[turn_number, (col + 1) // 2]
            target = col_land_ref.at[turn_number, (1 - col) // 2]
        else:
            source = row_send_ref.at[turn_number, (row + 1) // 2, per_row * ((col + 1) // 2)]
            target = corner_land_ref.at[turn_number, (1 - row) // 2, (1 - col) // 2]
        return pltpu.make_async_remote_copy(
            src_ref=source,
            dst_ref=target,
            send_sem=halo_sems.at[0, turn_number, which],
            recv_sem=halo_sems.at[1, turn_number, SIDES.index((-row, -col))],
            device_id=at(SIDES[which]),
            device_id_type=pl.DeviceIdType.MESH,
        )

    def share_edges(number):
        own = field_ref.at[number]
        for end in range(2):
            col_send_ref[number, end] = flat_strip(own, per_row * end)
        for which in (2, 3):
            pl.when(has(SIDES[which]))(lambda which=which: halo_copy(number, which).start())
        for end in range(2):
            for col in range(per_row + 1):
                row_send_ref[number, end, col] = own[col, TILE * end : TILE * end + EDGE].astype(WIRE)
        for which in (4, 5, 6, 7, 0, 1):
            pl.when(has(SIDES[which]))(lambda which=which: halo_copy(number, which).start())

    def take_edges(number):
        own = field_ref.at[number]

        def land(which):
            row, col = SIDES[which]
            halo_copy(number, which).wait_send()
            back = SIDES.index((row, col))
            pltpu.make_async_remote_copy(
                src_ref=halo_source(which),
                dst_ref=halo_target(which),
                send_sem=halo_sems.at[0, number, which],
                recv_sem=halo_sems.at[1, number, back],
                device_id=at(SIDES[which]),
                device_id_type=pl.DeviceIdType.MESH,
            ).wait_recv()
            if col == 0:
                end = (row + 1) // 2
                for tile in range(per_row + 1):
                    own[tile, TILE * end : TILE * end + EDGE] += row_land_ref[number, end, tile].astype(
                        jnp.float32
                    )
            elif row == 0:
                end = (col + 1) // 2
                add_flat(own, per_row * end, col_land_ref[number, end])
            else:
                end, tile = (row + 1) // 2, per_row * ((col + 1) // 2)
                value = corner_land_ref[number, end, (col + 1) // 2].astype(jnp.float32)
                inside = lanes_of(value.shape) < EDGE
                own[tile, TILE * end : TILE * end + EDGE] += jnp.where(inside, value, 0.0)

        def halo_source(which):
            row, col = SIDES[which]
            if col == 0:
                return row_send_ref.at[number, (row + 1) // 2]
            if row == 0:
                return col_send_ref.at[number, (col + 1) // 2]
            return row_send_ref.at[number, (row + 1) // 2, per_row * ((col + 1) // 2)]

        def halo_target(which):
            row, col = SIDES[which]
            if col == 0:
                return row_land_ref.at[number, (row + 1) // 2]
            if row == 0:
                return col_land_ref.at[number, (col + 1) // 2]
            return corner_land_ref.at[number, (row + 1) // 2, (col + 1) // 2]

        for which in range(len(SIDES)):
            pl.when(has(SIDES[which]))(functools.partial(land, which))

    def clear_outside(number):
        own = field_ref.at[number]

        @pl.when(ty == 0)
        def _():
            for tile in range(per_row + 1):
                own[tile, :MARGIN] = jnp.zeros((MARGIN, LANES), jnp.float32)

        @pl.when(ty == ty_size - 1)
        def _():
            for tile in range(per_row + 1):
                own[tile, TILE + MARGIN : EXTENT] = jnp.zeros((MARGIN, LANES), jnp.float32)

        @pl.when(tx == 0)
        def _():
            value = own[0, :EXTENT]
            own[0, :EXTENT] = jnp.where(lanes_of(value.shape) < MARGIN, 0.0, value)

        @pl.when(tx == tx_size - 1)
        def _():
            value = own[per_row, :EXTENT]
            own[per_row, :EXTENT] = jnp.where(lanes_of(value.shape) < MARGIN, value, 0.0)

    def gather_field(number):
        assemble(running_ref, index_smem, per_row, field_ref.at[number])
        share_edges(number)

    def damp(number):
        for tile in range(per_row + 1):
            field_ref[number, tile, :EXTENT] += damping * field_ref[number - 1, tile, :EXTENT]

    def forward(row, place, lane):
        cell = order_smem[2, place]
        matrix = matrix_ref[order_smem[1, place]]
        modelled = blur(shifted_ref, jnp.maximum(cell, 0) * 4, matrix, joined_ref.at[lane])
        squares = modelled * modelled
        squares = squares.reshape(block // 8, 8, LANES).sum(axis=0)
        sums_ref[row] += jnp.where(cell >= 0, squares, 0.0)
        hold_turns(modelled.astype(jnp.bfloat16).astype(jnp.float32), turned_ref.at[lane])

    def backward(place, lane):
        kept = same(place)
        matrix = matrix_ref[order_smem[1, place]]
        left, right = blur_back(turned_ref.at[lane], matrix, behind_ref.at[lane])
        running_ref[place + 1, 0] = left + jnp.where(kept, running_ref[place, 0], 0.0)
        running_ref[place + 1, 1] = right + jnp.where(kept, running_ref[place, 1], 0.0)

    def normal_pass(row, between):
        for lane in range(CAP):
            forward(row, lane, lane)

        @pl.loop(1, slots // CAP)
        def _(step):
            for lane in range(CAP):
                backward(CAP * (step - 1) + lane, lane)
            for lane in range(CAP):
                forward(row, CAP * step + lane, lane)

        between()
        for lane in range(CAP):
            backward(slots - CAP + lane, lane)

    gather_field(0)
    take_edges(0)
    clear_outside(0)
    shift_field(field_ref.at[0], shifted_ref, per_row, sums_ref, 0)
    normal_pass(1, lambda: None)
    gather_field(1)
    take_edges(1)
    clear_outside(1)
    damp(1)
    shift_field(field_ref.at[1], shifted_ref, per_row, sums_ref, 2)
    def sum_copy(step):
        peer = lax.rem(ty * tx_size + tx + step, ty_size * tx_size)
        return pltpu.make_async_remote_copy(
            src_ref=total_ref,
            dst_ref=total_land_ref.at[step],
            send_sem=sum_sems.at[0, step],
            recv_sem=sum_sems.at[1, step],
            device_id={"ty": peer // tx_size, "tx": lax.rem(peer, tx_size)},
            device_id_type=pl.DeviceIdType.MESH,
        )

    def send_sums():
        packed = jnp.zeros((1, LANES), jnp.float32)
        for number in range(4):
            value = jnp.sum(sums_ref[number], axis=0, keepdims=True)
            value = jnp.sum(value, axis=1, keepdims=True)
            packed = jnp.where(lanes_of(packed.shape) == number, value, packed)
        total_ref[...] = packed
        total_land_ref[0] = packed

        @pl.loop(1, ty_size * tx_size)
        def _(step):
            sum_copy(step).start()

    normal_pass(3, send_sums)
    gather_field(2)
    take_edges(2)
    damp(2)

    @pl.loop(1, ty_size * tx_size)
    def _(step):
        sum_copy(step).wait()

    total = total_land_ref[0]
    for step in range(1, ty_size * tx_size):
        total = total + total_land_ref[step]
    wide = jnp.zeros((1, LANES), jnp.float32)
    sums = [
        wide + jnp.sum(jnp.where(lanes_of(wide.shape) == number, total, 0.0), axis=1, keepdims=True)
        for number in range(4)
    ]
    r00 = sums[0]
    r01 = sums[1] + damping * r00
    r11 = sums[2]
    r12 = sums[3] + damping * r11
    step0 = r00 / r01
    norm_next = r00 - 2.0 * step0 * r01 + step0 * step0 * r11
    grown = 1.0 + norm_next / r00
    curvature = grown * grown * r01 - 2.0 * grown * step0 * r11 + step0 * step0 * r12
    step1 = norm_next / curvature
    x0 = step0 + step1 * grown
    x1 = -step1 * step0
    y1 = -step0 - step1 * grown
    y2 = step1 * step0

    chunk = 128

    @pl.loop(0, TILE // chunk)
    def _(number):
        start = pl.multiple_of(number * chunk, chunk)
        source = pl.ds(pl.multiple_of(start + MARGIN, 8), chunk)
        inside = lanes_of((chunk, LANES)) < LANES - MARGIN
        solved, left = [], []
        for tile in range(per_row + 1):
            q0, q1, q2 = (field_ref[k, tile, source] for k in range(3))
            solved.append(turn(x0 * q0 + x1 * q1, -MARGIN))
            left.append(turn(q0 + y1 * q1 + y2 * q2, -MARGIN))
        for tile in range(per_row):
            lanes = slice(tile * LANES, (tile + 1) * LANES)
            solution_ref[pl.ds(start, chunk), lanes] = jnp.where(inside, solved[tile], solved[tile + 1])
            residual_ref[pl.ds(start, chunk), lanes] = jnp.where(inside, left[tile], left[tile + 1])


def body(exposures, point_spread, warp_steps, column, block_cell):
    ty_size, tx_size = lax.axis_size("ty"), lax.axis_size("tx")
    frame_count, block = exposures.shape[:2]
    per_row = TILE // block
    slots = CAP * tx_size
    tall = EXTENT + 8
    f32, bf16 = jnp.float32, jnp.bfloat16
    vmem = pl.BlockSpec(memory_space=pltpu.VMEM)
    smem = pl.BlockSpec(memory_space=pltpu.SMEM)
    dma = pltpu.SemaphoreType.DMA
    scratch = [
        pltpu.VMEM((GROUP, frame_count, LANES), f32),
        pltpu.VMEM((frame_count, 16, LANES), bf16),
        pltpu.VMEM((tx_size, CAP, ROWS, LANES), bf16),
        pltpu.VMEM((tx_size, CAP, ROWS, LANES), bf16),
        pltpu.VMEM((tx_size, 8, LANES), jnp.int32),
        pltpu.VMEM((tx_size, 8, LANES), jnp.int32),
        pltpu.SMEM((tx_size, 8, LANES), jnp.int32),
        pltpu.SMEM((slots,), jnp.int32),
        pltpu.SMEM((3, slots), jnp.int32),
        pltpu.SMEM((per_row * per_row,), jnp.int32),
        pltpu.VMEM((slots, 256, 256), bf16),
        pltpu.VMEM((slots, 2, PATCH, LANES), f32),
        pltpu.VMEM((slots + 1, 2, PATCH, LANES), f32),
        pltpu.VMEM((CAP, 4, PAD + ROWS, LANES), f32),
        pltpu.VMEM((CAP, 2, 8 + PATCH, LANES), f32),
        pltpu.VMEM((CAP, 4, ROWS - 8, LANES), f32),
        pltpu.VMEM((4 * per_row * per_row, PATCH, LANES), bf16),
        pltpu.VMEM((3, per_row + 1, tall, LANES), f32),
        pltpu.VMEM((3, 2, per_row + 1, EDGE, LANES), WIRE),
        pltpu.VMEM((3, 2, EXTENT // 4, LANES), WIRE),
        pltpu.VMEM((3, 2, per_row + 1, EDGE, LANES), WIRE),
        pltpu.VMEM((3, 2, EXTENT // 4, LANES), WIRE),
        pltpu.VMEM((3, 2, 2, EDGE, LANES), WIRE),
        pltpu.VMEM((4, 8, LANES), f32),
        pltpu.VMEM((1, LANES), f32),
        pltpu.VMEM((ty_size * tx_size, 1, LANES), f32),
        dma((2, tx_size)),
        dma((2, tx_size)),
        dma,
        dma((2, 3, len(SIDES))),
        dma((2, ty_size * tx_size)),
    ]
    return pl.pallas_call(
        functools.partial(whole_kernel, (ty_size, tx_size)),
        out_shape=(jax.ShapeDtypeStruct((TILE, TILE), f32), jax.ShapeDtypeStruct((TILE, TILE), f32)),
        in_specs=[vmem, vmem, smem, smem, smem],
        out_specs=(vmem, vmem),
        scratch_shapes=scratch,
        compiler_params=pltpu.CompilerParams(
            collective_id=0, has_side_effects=True, vmem_limit_bytes=36 * 1024 * 1024
        ),
        name="whole",
    )(exposures, point_spread.transpose(1, 0, 2), warp_steps.T, column[:, 0], block_cell)


def solution(mesh):
    placed = (
        P(("ty", "tx"), None, None),
        P(("ty", "tx"), None, None),
        P(("ty", "tx"), None),
        P(("ty", "tx"), None),
        P(("ty", "tx")),
    )
    return jax.shard_map(
        body, mesh=mesh, in_specs=placed, out_specs=(P("ty", "tx"), P("ty", "tx")), check_vma=False
    )
```
